32 devices in a mesh: gx: 4 (over z), gy: 8 (over y, x, core).
Axes of the slice: x: 2, y: 2, z: 4, core: 2. Of those that a mesh axis runs over, the one named last changes fastest.
Arguments:
- matrix_rows: float32 [4096, 1024], P(('gx', 'gy')), may hold values from -1.1 to 1.1
- tile_owner: int32 [136], replicated, may hold values from 0 to 31, as said below
- tile_slot: int32 [136], replicated, may hold values from 0 to 4, as said below
Outputs:
- packed_tiles: float32 [160, 256, 256], P(('gx', 'gy'))
The draws below stay inside these ranges and needn't reach their ends.
Inputs may be any that keep to these rules, and one draw needn't show every extreme that they name: `tile_owner`: give tile (I, J) the class (c, r) as follows, with a = I // 4, b = J // 4, i = I % 4, j = J % 4: if a == b, c = a and r = i when i - j < 2, else r = j; if a > b and (a - b > 2, or a - b == 2 with i + j even), c = b and r = i; otherwise c = a and r = j. The owner of a class (c, r) tile is one of the devices c * 8 to c * 8 + 7. Every owner holds 4 or 5 tiles. At most 2 tiles of one class share an owner, and in every draw some owner holds exactly 2 tiles of one class. `tile_slot`: the tiles of one owner take the slots 0 to their count - 1, each once.
All inputs are finite; a program needn't handle non-finite values.
Results may differ from the reference program's by a relative error of at most 0.0003.
Values sent between devices are 32-bit elements; how exact they have to be, the bound alone decides.
No kernel may reach another device: no remote copies, remote signals or barrier semaphores. Data moves between devices by JAX's collectives and lax.ppermute only.
A program may use at most 128 MiB of HBM per device.

```python
import jax
import jax.numpy as jnp
import numpy as np
from jax import lax

WIDTH = 1024
TILE = 256
ORDER = 4096
TILE_COUNT = 16
HALF_TILES = 4
LOWER_COUNT = 136
SLOTS = 5
N_GX = 4
N_GY = 8
DEVICES = 32


def tile_classes():
    lower_i, lower_j = np.tril_indices(TILE_COUNT)
    group_a = lower_i // HALF_TILES
    group_b = lower_j // HALF_TILES
    inner_i = lower_i % HALF_TILES
    inner_j = lower_j % HALF_TILES
    same = group_a == group_b
    within_row = inner_i - inner_j < HALF_TILES // 2
    gap = group_a - group_b
    across_row = (gap > N_GX // 2) | (gap == N_GX // 2) & ((inner_i + inner_j) % 2 == 0)
    rowwise = np.where(same, within_row, across_row)
    class_x = np.where(same | ~rowwise, group_a, group_b)
    class_r = np.where(rowwise, inner_i, inner_j)
    return (class_x.astype(np.int32), class_r.astype(np.int32))


def owner_table(key):
    class_x, class_r = tile_classes()
    set_id = jnp.asarray(class_x * HALF_TILES + class_r, jnp.int32)
    row_of = jnp.asarray(class_x, jnp.int32)
    set_rank = jax.random.permutation(jax.random.fold_in(key, 11), TILE_COUNT).astype(jnp.int32)
    tile_rank = jax.random.permutation(jax.random.fold_in(key, 12), LOWER_COUNT).astype(jnp.int32)
    score = (row_of * TILE_COUNT + set_rank[set_id]) * LOWER_COUNT + tile_rank
    order = jnp.argsort(score, stable=True).astype(jnp.int32)
    position = jnp.zeros((LOWER_COUNT,), jnp.int32).at[order].set(jnp.arange(LOWER_COUNT, dtype=jnp.int32))
    per_row = LOWER_COUNT // N_GX
    inside_row = position % per_row
    row_keys = jax.random.split(jax.random.fold_in(key, 13), N_GX)
    owner_order = jax.vmap(lambda one: jax.random.permutation(one, N_GY))(row_keys).astype(jnp.int32)
    owners = row_of * N_GY + owner_order[row_of, inside_row % N_GY]
    slot_index = inside_row // N_GY
    return (owners.astype(jnp.int32), slot_index.astype(jnp.int32))


def draw_tile_owner(key, part):
    return owner_table(key)[0]


def draw_tile_slot(key, part):
    return owner_table(key)[1]


def shard_levels(own_key, dims, shards, smallest, largest):
    def one(dim, shards_of):
        heights = jax.random.uniform(jax.random.fold_in(jax.random.fold_in(own_key, 6), dim), (shards_of,), jnp.float32, smallest / len(shards), largest / len(shards))
        return jnp.repeat(jnp.exp(heights), dims[dim] // shards_of).reshape((-1,) + (1,) * (len(dims) - dim - 1))

    level = one(*shards[0])
    for cut in shards[1:]:
        level = level * one(*cut)
    return level


def normal_values(stream_key, extent, width, limit, pieces=(), kind=jnp.bfloat16):
    gain = shard_levels(stream_key, extent, pieces, -0.22, 0.18) if pieces else 1.0
    values = jax.random.normal(stream_key, extent, jnp.float32) * width * gain
    return jnp.minimum(jnp.maximum(values, -limit), limit).astype(kind)


def setup_inputs(seed: int = 0) -> dict:
    splits = jax.random.split(jax.random.key(seed), 4)
    matrix_rows = normal_values(splits[0], (ORDER, WIDTH), 0.177, 1.1, ((0, 32),), jnp.float32)
    tile_owner = draw_tile_owner(jax.random.fold_in(splits[3], 71), 0)
    tile_slot = draw_tile_slot(jax.random.fold_in(splits[3], 71), 0)
    return dict(matrix_rows=matrix_rows, tile_owner=tile_owner, tile_slot=tile_slot)


def reference(matrix_rows, tile_owner, tile_slot):
    lower_i, lower_j = np.tril_indices(TILE_COUNT)
    row_table = jnp.asarray(lower_i, jnp.int32)
    col_table = jnp.asarray(lower_j, jnp.int32)
    blocks = matrix_rows.reshape(TILE_COUNT, TILE, WIDTH)
    inside = lax.broadcasted_iota(jnp.int32, (TILE, TILE), 0)
    across = lax.broadcasted_iota(jnp.int32, (TILE, TILE), 1)

    def one_tile(index):
        row_tile = row_table[index]
        col_tile = col_table[index]
        product = lax.dot_general(blocks[row_tile], blocks[col_tile], (((1,), (1,)), ((), ())),
                                  precision=lax.Precision.HIGHEST, preferred_element_type=jnp.float32)
        upper = jnp.logical_and(row_tile == col_tile, inside < across)
        return jnp.where(upper, jnp.float32(0.0), product)

    tiles = lax.map(one_tile, jnp.arange(LOWER_COUNT, dtype=jnp.int32))
    packed = jnp.zeros((DEVICES, SLOTS, TILE, TILE), jnp.float32)
    packed = packed.at[tile_owner, tile_slot].set(tiles)
    return packed.reshape(DEVICES * SLOTS, TILE, TILE)
```

```python
import functools

import jax
import jax.numpy as jnp
from jax import lax
from jax.experimental import pallas as pl
from jax.experimental.pallas import tpu as pltpu
from jax.sharding import PartitionSpec as P

CHUNKS = 2


def plan_rounds(shifts, classes):
    bits = []
    while 1 << len(bits) < classes:
        bits.append(1 << len(bits))
    assert 1 << len(bits) == classes
    every = [(s, k) for s in range(shifts + 1) for k in range(classes)]
    have = {(0, 0)}
    rounds = []
    while len(have) < len(every):
        hops = []
        taken = set()
        for direction in ["x"] + bits:
            options = []
            for s, k in every:
                if (s, k) in have or (s, k) in taken:
                    continue
                source = (s - 1, k) if direction == "x" else (s, k ^ direction)
                if source in have:
                    options.append((bin(k).count("1"), s, k))
            if options:
                _, s, k = min(options)
                taken.add((s, k))
                hops.append((direction, s, k))
        have |= taken
        rounds.append(hops)
    return rounds


def tiles_kernel(late, slots, table, *refs):
    own_h = lax.axis_index("gy") % 2
    blocks = refs[: len(refs) - 7 + (0 if late else 1)]
    rest = refs[len(blocks):]
    if late:
        _, out, left, right, result, load_sem, store_sem = rest
    else:
        out, left, right, result, load_sem, store_sem = rest
    parts = 2 * CHUNKS
    count = len(blocks) // parts
    rows = left.shape[1] // parts

    def place(slot, field):
        return table[slot * 6 + field]

    def copies(which, buffer, ref, sem, block):
        for half in range(2):
            for chunk in range(CHUNKS):
                side = own_h if half == 0 else 1 - own_h
                start = pl.multiple_of((side * CHUNKS + chunk) * rows, rows)
                yield pltpu.make_async_copy(
                    blocks[block * parts + half * CHUNKS + chunk],
                    ref.at[buffer, pl.ds(start, rows), :],
                    load_sem.at[buffer, sem],
                )

    def load(slot, buffer):
        for field, ref, sem in ((1, left, 0), (2, right, 1)):
            for block in range(count):
                @pl.when(place(slot, field) == block)
                def _():
                    for copy in copies(field, buffer, ref, sem, block):
                        copy.start()

    def arrive(buffer):
        for field, ref, sem in ((1, left, 0), (2, right, 1)):
            for copy in copies(field, buffer, ref, sem, 0):
                copy.wait()

    def store(slot):
        return pltpu.make_async_copy(result.at[slot], out.at[slot], store_sem.at[slot])

    def active(slot):
        return place(slot, 4) == (1 if late else 0)

    @pl.when(active(0))
    def _():
        load(0, 0)

    def step(slot, carry):
        buffer = lax.rem(slot, 2)
        following = jnp.minimum(slot + 1, slots - 1)

        @pl.when(jnp.logical_and(slot + 1 < slots, active(following)))
        def _():
            load(following, 1 - buffer)

        @pl.when(active(slot))
        def _():
            arrive(buffer)
            size, width = left.shape[1], left.shape[2]
            depth = min(width, 512)
            total = jnp.zeros((size, size), jnp.float32)
            dims = (((1,), (1,)), ((), ()))
            for start in range(0, width, depth):
                a = left[buffer, :, start : start + depth]
                b = right[buffer, :, start : start + depth]
                a_hi = a.astype(jnp.bfloat16)
                b_hi = b.astype(jnp.bfloat16)
                a_lo = (a - a_hi.astype(jnp.float32)).astype(jnp.bfloat16)
                b_lo = (b - b_hi.astype(jnp.float32)).astype(jnp.bfloat16)
                dot = functools.partial(
                    lax.dot_general, dimension_numbers=dims, preferred_element_type=jnp.float32
                )
                total = total + dot(a_hi, b_hi) + (dot(a_hi, b_lo) + dot(a_lo, b_hi))
            inside = lax.broadcasted_iota(jnp.int32, (size, size), 0)
            across = lax.broadcasted_iota(jnp.int32, (size, size), 1)
            above = jnp.logical_and(place(slot, 3) == 1, inside < across)
            result[slot] = jnp.where(above, 0.0, total)
            store(slot).start()

        if not late:
            @pl.when(place(slot, 4) == 2)
            def _():
                result[slot] = jnp.zeros(result.shape[1:], jnp.float32)
                store(slot).start()

        return carry

    lax.fori_loop(0, slots, step, 0)

    def finish(slot, carry):
        started = active(slot) if late else place(slot, 4) != 1

        @pl.when(started)
        def _():
            store(slot).wait()

        return carry

    lax.fori_loop(0, slots, finish, 0)


def compute_tiles(table, blocks, slots, size, width, previous=None):
    late = previous is not None
    anywhere = pl.BlockSpec(memory_space=pltpu.HBM)
    operands = [table] + blocks + ([previous] if late else [])
    return pl.pallas_call(
        functools.partial(tiles_kernel, late, slots),
        out_shape=jax.ShapeDtypeStruct((slots, size, size), jnp.float32),
        in_specs=[pl.BlockSpec(memory_space=pltpu.SMEM)] + [anywhere] * (len(operands) - 1),
        out_specs=anywhere,
        scratch_shapes=[
            pltpu.VMEM((2, size, width), jnp.float32),
            pltpu.VMEM((2, size, width), jnp.float32),
            pltpu.VMEM((slots, size, size), jnp.float32),
            pltpu.SemaphoreType.DMA((2, 2)),
            pltpu.SemaphoreType.DMA((slots,)),
        ],
        input_output_aliases={len(operands) - 1: 0} if late else {},
        cost_estimate=pl.CostEstimate(
            flops=6 * slots * size * size * width,
            bytes_accessed=8 * slots * size * width,
            transcendentals=0,
        ),
        compiler_params=pltpu.CompilerParams(vmem_limit_bytes=32 * 1024 * 1024),
        name="late_tiles" if late else "early_tiles",
    )(*operands)


def slot_table(tile_owner, tile_slot, slots, classes, count_x, x_index, y_index, late_blocks):
    lower_count = tile_owner.shape[0]
    count_y = 2 * classes
    tile_count = count_x * classes
    own_r = y_index // 2
    me = x_index * count_y + y_index
    number = lax.broadcasted_iota(jnp.int32, (slots, lower_count), 1)
    slot = lax.broadcasted_iota(jnp.int32, (slots, lower_count), 0)
    mine = jnp.logical_and(tile_owner[None, :] == me, tile_slot[None, :] == slot)
    tile = jnp.sum(jnp.where(mine, number + 1, 0), axis=1, dtype=jnp.int32)
    present = tile > 0
    tile = jnp.maximum(tile - 1, 0)
    starts = lax.broadcasted_iota(jnp.int32, (slots, tile_count - 1), 1) + 1
    starts = starts * (starts + 1) // 2
    row = jnp.sum((tile[:, None] >= starts).astype(jnp.int32), axis=1, dtype=jnp.int32)
    col = tile - row * (row + 1) // 2

    def block(index):
        shift = (x_index - index // classes) % count_x
        return shift * classes + ((index % classes) ^ own_r)

    row_block = block(row)
    col_block = block(col)
    late = jnp.zeros_like(present)
    for q in late_blocks:
        late = late | (row_block == q) | (col_block == q)
    stage = jnp.where(present, late.astype(jnp.int32), 2)
    diagonal = (row == col).astype(jnp.int32)
    fields = [present.astype(jnp.int32), row_block, col_block, diagonal, stage, stage]
    return jnp.stack(fields, axis=1).reshape(-1)


def per_device(matrix_rows, tile_owner, tile_slot):
    rows_dev, width = matrix_rows.shape
    size = 2 * rows_dev
    count_x = lax.axis_size("gx")
    count_y = lax.axis_size("gy")
    classes = count_y // 2
    shifts = count_x // 2
    devices = count_x * count_y
    slots = (tile_owner.shape[0] + devices - 1) // devices
    x_index = lax.axis_index("gx")
    y_index = lax.axis_index("gy")
    rounds = plan_rounds(shifts, classes)
    part = rows_dev // CHUNKS

    def hop(value, direction):
        if direction == "x":
            pairs = [(source, (source + 1) % count_x) for source in range(count_x)]
            return lax.ppermute(value, "gx", pairs)
        flip = 1 if direction == "core" else 2 * direction
        return lax.ppermute(value, "gy", [(source, source ^ flip) for source in range(count_y)])

    own = {}
    other = {}
    for chunk in range(CHUNKS):
        own[0, 0, chunk] = matrix_rows[chunk * part : (chunk + 1) * part]
        other[0, 0, chunk] = hop(own[0, 0, chunk], "core")
    for hops in rounds:
        for chunk in range(CHUNKS):
            for direction, s, k in hops:
                source = (s - 1, k) if direction == "x" else (s, k ^ direction)
                own[s, k, chunk] = hop(own[source + (chunk,)], direction)
                other[s, k, chunk] = hop(own[s, k, chunk], "core")

    late_blocks = [s * classes + k for _, s, k in rounds[-1]]
    table = slot_table(
        tile_owner, tile_slot, slots, classes, count_x, x_index, y_index, late_blocks
    )

    def operands(skip):
        arrays = []
        for s in range(shifts + 1):
            for k in range(classes):
                if s * classes + k in skip:
                    arrays += [own[0, 0, chunk] for chunk in range(CHUNKS)] * 2
                    continue
                arrays += [own[s, k, chunk] for chunk in range(CHUNKS)]
                arrays += [other[s, k, chunk] for chunk in range(CHUNKS)]
        return arrays

    early = compute_tiles(table, operands(late_blocks), slots, size, width)
    return compute_tiles(table, operands([]), slots, size, width, early)


def solution(mesh):
    placed = (P(("gx", "gy"), None), P(), P())
    return jax.shard_map(
        per_device,
        mesh=mesh,
        in_specs=placed,
        out_specs=P(("gx", "gy"), None, None),
        check_vma=False,
    )
```
